32 devices in a mesh: section: 4 (over y, x), mp: 8 (over z, core).
Axes of the slice: x: 2, y: 2, z: 4, core: 2. Of those that a mesh axis runs over, the one named last changes fastest.
Arguments:
- hidden_in: bfloat16 [1, 4, 64, 4096], P(None, 'section'), may hold values from -36 to 36
- attn_gain: bfloat16 [4, 4096], P('section'), may hold values from 0.5 to 2
- w_query: bfloat16 [4, 4096, 4096], P('section', None, 'mp'), may hold values from -0.75 to 0.75
- w_key: bfloat16 [4, 4096, 1024], P('section', None, 'mp'), may hold values from -0.0625 to 0.0625
- w_value: bfloat16 [4, 4096, 1024], P('section', None, 'mp'), may hold values from -0.09375 to 0.09375
- w_out: bfloat16 [4, 4096, 4096], P('section', 'mp'), may hold values from -0.09375 to 0.09375
- ffn_gain: bfloat16 [4, 4096], P('section'), may hold values from 0.5 to 2
- w_gate: bfloat16 [4, 4096, 14336], P('section', None, 'mp'), may hold values from -0.09375 to 0.09375
- w_up: bfloat16 [4, 4096, 14336], P('section', None, 'mp'), may hold values from -0.09375 to 0.09375
- w_down: bfloat16 [4, 14336, 4096], P('section', 'mp'), may hold values from -0.046875 to 0.046875
- ffn_blocks: int32 [4, 4], P(None, 'section'), may hold values from 1 to 112
- heads_on: int32 [4, 4], P(None, 'section'), may hold values from 1 to 32
Outputs:
- hidden_out: bfloat16 [1, 4, 64, 4096], P(None, 'section')
The draws below stay inside these ranges and needn't reach their ends.
Inputs may be any that keep to these rules, and one draw needn't show every extreme that they name: `ffn_blocks`: hidden units below 128 times the entry are active. `heads_on`: query heads below the entry are active.
All inputs are finite; a program needn't handle non-finite values.
Results may differ from the reference program's by a relative error of at most 0.025.
Values may be sent and summed in bfloat16 or wider, within the bound.
No kernel may reach another device: no remote copies, remote signals or barrier semaphores. Data moves between devices by JAX's collectives and lax.ppermute only.
A program may use at most 128 MiB of HBM per device.

```python
import math
import jax
import jax.numpy as jnp
from jax import lax

D = 4096
HEADS = 32
KV_HEADS = 8
HD = 128
BLOCK = 128
FFB = 112
FF = 14336
FFP = 14336
SECTIONS = 4
LAYERS = 4
LEN = 64
MICRO_DEV = 1
MICRO = 4
N_MP = 8


def query_key_pair(key):
    folded = jax.random.fold_in(key, 7101)
    key_keys, key_query = jax.random.split(folded, 2)
    query_shape = (LAYERS, D, HEADS * HD)
    key_shape = (LAYERS, D, KV_HEADS * HD)
    spread_scale = D ** (-0.5)
    key_weight = jnp.clip(jax.random.normal(key_keys, key_shape, jnp.float32), -4.0, 4.0) * spread_scale
    query_weight = jnp.clip(jax.random.normal(key_query, query_shape, jnp.float32), -4.0, 4.0) * spread_scale
    return (query_weight, key_weight)


def draw_w_query(key, part):
    return query_key_pair(key)[0].astype(jnp.bfloat16)


def draw_w_key(key, part):
    return query_key_pair(key)[1].astype(jnp.bfloat16)


def draw_hidden_in(key, part):
    folded = jax.random.fold_in(key, 7202)
    key_noise, key_rows, key_columns = jax.random.split(folded, 3)
    array_shape = (MICRO_DEV, SECTIONS, LEN, D)
    low_end = jnp.log(0.3)
    high_end = jnp.log(3.0)
    row_scale = jnp.exp(jax.random.uniform(key_rows, (MICRO_DEV, SECTIONS, LEN, 1), jnp.float32, low_end, high_end))
    col_scale = jnp.exp(jax.random.uniform(key_columns, (1, 1, 1, D), jnp.float32, low_end, high_end))
    jitter = jnp.clip(jax.random.normal(key_noise, array_shape, jnp.float32), -4.0, 4.0)
    return (jitter * row_scale * col_scale).astype(jnp.bfloat16)


def place_ends(array, stream_key, least, high):
    index_at = [jax.random.randint(jax.random.fold_in(stream_key, axis), (), 0, length) for axis, length in enumerate(array.shape)]
    longest = array.shape.index(max(array.shape))
    next_to = index_at[:longest] + [(index_at[longest] + 1) % array.shape[longest]] + index_at[longest + 1:]
    return array.at[tuple(index_at)].set(least).at[tuple(next_to)].set(high)


def shard_levels(stream_key, shape, pieces, smallest, top_value):
    factor_of = 1.0
    for dim, shards_of in pieces:
        steps = jax.random.uniform(jax.random.fold_in(jax.random.fold_in(stream_key, 6), dim), (shards_of,), jnp.float32, smallest / len(pieces), top_value / len(pieces))
        factor_of = factor_of * jnp.repeat(jnp.exp(steps), shape[dim] // shards_of).reshape((-1,) + (1,) * (len(shape) - 1 - dim))
    return factor_of


def centred(key, extent, width, reach, pieces=(), held_as=jnp.bfloat16):
    factor_of = shard_levels(key, extent, pieces, -0.22, 0.18) if pieces else 1.0
    values = jax.random.normal(key, extent, jnp.float32) * width * factor_of
    return jnp.minimum(jnp.maximum(values, -reach), reach).astype(held_as)


def setup_inputs(seed: int = 0) -> dict:
    keys = jax.random.split(jax.random.key(seed), 13)
    hidden_in = draw_hidden_in(jax.random.fold_in(keys[12], 71), 0)
    attn_gain = jnp.clip(jnp.exp(math.log(2.0) - 1.3862944 * jax.random.uniform(keys[1], (LAYERS, D), jnp.float32) ** shard_levels(keys[1], (LAYERS, D), ((0, 4),), -0.2, 0.2)), 0.5, 2.0).astype(jnp.bfloat16)
    w_query = draw_w_query(jax.random.fold_in(keys[12], 71), 0)
    w_key = draw_w_key(jax.random.fold_in(keys[12], 71), 0)
    w_value = centred(keys[4], (LAYERS, D, KV_HEADS * HD), D ** -0.5, 0.09375, ((0, 4), (2, 8)))
    w_out = centred(keys[5], (LAYERS, HEADS * HD, D), (HEADS * HD) ** -0.5, 0.09375, ((0, 4), (1, 8)))
    ffn_gain = jnp.clip(jnp.exp(math.log(2.0) - 1.3862944 * jax.random.uniform(keys[6], (LAYERS, D), jnp.float32) ** shard_levels(keys[6], (LAYERS, D), ((0, 4),), -0.2, 0.2)), 0.5, 2.0).astype(jnp.bfloat16)
    w_gate = centred(keys[7], (LAYERS, D, FFP), D ** -0.5, 0.09375, ((0, 4), (2, 8)))
    w_up = centred(keys[8], (LAYERS, D, FFP), D ** -0.5, 0.09375, ((0, 4), (2, 8)))
    w_down = centred(keys[9], (LAYERS, FFP, D), FF ** -0.5, 0.046875, ((0, 4), (1, 8)))
    ffn_blocks = place_ends(jax.random.randint(keys[10], (MICRO, LAYERS), 1, FFB + 1), jax.random.fold_in(keys[10], 1), 1, FFB).astype(jnp.int32)
    heads_on = place_ends(jax.random.randint(keys[11], (MICRO, LAYERS), 1, HEADS + 1), jax.random.fold_in(keys[11], 1), 1, HEADS).astype(jnp.int32)
    return {"hidden_in": hidden_in, "attn_gain": attn_gain, "w_query": w_query, "w_key": w_key, "w_value": w_value, "w_out": w_out, "ffn_gain": ffn_gain, "w_gate": w_gate, "w_up": w_up, "w_down": w_down, "ffn_blocks": ffn_blocks, "heads_on": heads_on}


ROPE_BASE = 500000.0
EPSILON = 1e-05

def rms_scale(values, gain_row):
    mean_sq = lax.optimization_barrier(jnp.mean(values * values, axis=-1, keepdims=True))
    return values * lax.rsqrt(mean_sq + EPSILON) * gain_row.astype(jnp.float32)

def rotate(values):
    length = values.shape[0]
    half_dim = values.shape[-1] // 2
    frequency = ROPE_BASE ** (-(jnp.arange(half_dim, dtype=jnp.float32) / half_dim))
    angles = jnp.arange(length, dtype=jnp.float32)[:, None] * frequency[None, :]
    cosine_table = jnp.cos(angles)[:, None, :]
    sine_table = jnp.sin(angles)[:, None, :]
    front_half = values[..., :half_dim].astype(jnp.float32)
    back_half = values[..., half_dim:].astype(jnp.float32)
    return jnp.concatenate([front_half * cosine_table - back_half * sine_table, front_half * sine_table + back_half * cosine_table], axis=-1)

def group_sum(left, right):
    length, inner = left.shape
    group_width = inner // N_MP
    left_groups = left.reshape(length, N_MP, group_width).astype(jnp.float32)
    right_groups = right.reshape(N_MP, group_width, right.shape[1]).astype(jnp.float32)
    partials = jnp.einsum('tgk,gkd->gtd', left_groups, right_groups).astype(jnp.bfloat16)
    return lax.optimization_barrier(jnp.sum(partials.astype(jnp.float32), axis=0))

def layer_step(carried, layer_pos, active, block_count, attn_gain, w_query, w_key, w_value, w_out, ffn_gain, w_gate, w_up, w_down):
    length = carried.shape[0]
    group_size = HEADS // KV_HEADS
    residual = carried.astype(jnp.float32)
    normed = rms_scale(residual, attn_gain[layer_pos]).astype(jnp.bfloat16)
    queries = rotate(jnp.dot(normed, w_query[layer_pos], preferred_element_type=jnp.float32).reshape(length, HEADS, HD)).astype(jnp.bfloat16)
    key_proj = jnp.dot(normed, w_key[layer_pos], preferred_element_type=jnp.float32).astype(jnp.bfloat16).reshape(length, HD, KV_HEADS).transpose(0, 2, 1)
    keys_rot = rotate(key_proj).astype(jnp.bfloat16)
    values = jnp.dot(normed, w_value[layer_pos], preferred_element_type=jnp.float32).astype(jnp.bfloat16).reshape(length, HD, KV_HEADS).transpose(0, 2, 1)
    keys_all = jnp.repeat(keys_rot, group_size, axis=1)
    values_all = jnp.repeat(values, group_size, axis=1)
    scores = jnp.einsum('qhd,khd->hqk', queries.astype(jnp.float32), keys_all.astype(jnp.float32)) * HD ** (-0.5)
    causal = jnp.arange(length)[:, None] >= jnp.arange(length)[None, :]
    scores = jnp.where(causal[None], scores, -jnp.inf)
    probabilities = jax.nn.softmax(scores, axis=-1).astype(jnp.bfloat16)
    context = jnp.einsum('hqk,khd->qhd', probabilities.astype(jnp.float32), values_all.astype(jnp.float32))
    head_ids = jnp.arange(HEADS)
    context = jnp.where((head_ids < active)[None, :, None], context, 0.0).astype(jnp.bfloat16)
    attended = residual + group_sum(context.reshape(length, HEADS * HD), w_out[layer_pos])
    normed_ffn = rms_scale(attended, ffn_gain[layer_pos]).astype(jnp.bfloat16)
    gate_part = jnp.dot(normed_ffn, w_gate[layer_pos][:, :FF], preferred_element_type=jnp.float32)
    up_part = jnp.dot(normed_ffn, w_up[layer_pos][:, :FF], preferred_element_type=jnp.float32)
    unit_ids = jnp.arange(FF)
    hidden = jnp.where((unit_ids < BLOCK * block_count)[None, :], jax.nn.silu(gate_part) * up_part, 0.0).astype(jnp.bfloat16)
    padded = jnp.pad(hidden, ((0, 0), (0, w_gate.shape[2] - FF)))
    return (attended + group_sum(padded, w_down[layer_pos])).astype(jnp.bfloat16)

def reference(hidden_in, attn_gain, w_query, w_key, w_value, w_out, ffn_gain, w_gate, w_up, w_down, ffn_blocks, heads_on):
    finished = []
    for micro_index in range(MICRO):
        carried = hidden_in[micro_index // SECTIONS, micro_index % SECTIONS]
        for layer_pos in range(LAYERS):
            carried = layer_step(carried, layer_pos, heads_on[micro_index, layer_pos], ffn_blocks[micro_index, layer_pos], attn_gain, w_query, w_key, w_value, w_out, ffn_gain, w_gate, w_up, w_down)
        finished.append(carried)
    return jnp.stack(finished).reshape(MICRO_DEV, SECTIONS, LEN, D)
```

```python
import jax
import jax.numpy as jnp
from jax import lax
from jax.experimental import pallas as pl
from jax.experimental.pallas import tpu as pltpu
from jax.sharding import PartitionSpec as P

HEADS = 32
KV_HEADS = 8
HD = 128
BLOCK = 128
CORES = 2
LANES = 128

ROPE_BASE = 500000.0
EPSILON = 1e-05
GROUP = 1


F32 = jnp.float32
BF16 = jnp.bfloat16

VMEM = pl.BlockSpec(memory_space=pltpu.VMEM)
SMEM = pl.BlockSpec(memory_space=pltpu.SMEM)
ANY = pl.BlockSpec(memory_space=pl.ANY)
CORE, CHIP, SECTION, FIRST_HEAD, FIRST_UNIT = range(5)


def dot(left, right):
    return jnp.dot(left, right, preferred_element_type=F32)


def shaped(rows, columns, dtype=BF16):
    return jax.ShapeDtypeStruct((rows, columns), dtype)


def kernel_call(body, name, out_shape, in_specs, scratch=()):
    many = isinstance(out_shape, (list, tuple))
    return pl.pallas_call(
        body,
        out_shape=out_shape,
        in_specs=in_specs,
        out_specs=[VMEM] * len(out_shape) if many else VMEM,
        scratch_shapes=list(scratch),
        compiler_params=pltpu.CompilerParams(vmem_limit_bytes=4 << 20),
        name=name,
    )


def rope_tables(length):
    half_dim = HD // 2
    frequency = ROPE_BASE ** (-(jnp.arange(half_dim, dtype=F32) / half_dim))
    angles = jnp.arange(length, dtype=F32)[:, None] * frequency[None, :]
    cosine = jnp.cos(angles)
    sine = jnp.sin(angles)
    return (
        jnp.concatenate([cosine, cosine], axis=1),
        jnp.concatenate([-sine, sine], axis=1),
    )


def span_of(index, width):
    return pl.ds(pl.multiple_of(index * width, width), width)


def assemble(info, pieces, whole):
    chips = len(pieces) // CORES
    width = pieces[0].shape[1]
    for core_step in range(CORES):
        for step in range(chips):
            core = info[CORE] ^ core_step
            block = core * chips + (info[CHIP] ^ step)
            whole[:, span_of(block, width)] = pieces[core_step * chips + step][...]


def gain_rows(rows, gain, gained):
    columns = rows.shape[1]
    total = jnp.zeros((rows.shape[0], LANES), F32)
    for first in range(0, columns, LANES):
        at = slice(first, first + LANES)
        value = rows[:, at].astype(F32)
        total = total + value * value
        gained[:, at] = (value * gain[:, at]).astype(BF16)
    mean_sq = jnp.sum(total, axis=1, keepdims=True) / columns
    return lax.rsqrt(mean_sq + EPSILON)


def row_scale(gained, inverse_gain):
    columns = gained.shape[1]
    total = jnp.zeros((gained.shape[0], LANES), F32)
    for first in range(0, columns, LANES):
        at = slice(first, first + LANES)
        value = gained[:, at].astype(F32) * inverse_gain[:, at]
        total = total + value * value
    mean_sq = jnp.sum(total, axis=1, keepdims=True) / columns
    return lax.rsqrt(mean_sq + EPSILON)


def halves_dot(info, left, weights, theirs, mine, step):
    half = theirs.shape[1]
    step = min(step, half)
    for out, core in ((theirs, 1 - info[CORE]), (mine, info[CORE])):
        for n in range(half // step):
            at = span_of(core * (half // step) + n, step)
            out[:, n * step : (n + 1) * step] = dot(left[...], weights[:, at]).astype(BF16)


def load_body(*refs, many):
    sources = refs[-3 * many : -2 * many]
    targets = refs[-2 * many : -many]
    copies = [
        pltpu.make_async_copy(source.at[0], target, arrived)
        for source, target, arrived in zip(sources, targets, refs[-many:])
    ]
    for copy in copies:
        copy.start()
    for copy in copies:
        copy.wait()


def resident(arrays, after):
    many = len(arrays)

    def load(*refs):
        load_body(*refs, many=many)

    return pl.pallas_call(
        load,
        out_shape=[pltpu.VMEM(array.shape[1:], array.dtype) for array in arrays],
        in_specs=[ANY] * len(after) + [pl.BlockSpec(memory_space=pltpu.HBM)] * many,
        out_specs=[VMEM] * many,
        scratch_shapes=[pltpu.SemaphoreType.DMA] * many,
        compiler_params=pltpu.CompilerParams(vmem_limit_bytes=1 << 18),
        name="resident",
    )(*after, *arrays)


def cut_body(info, source, target, *, chips):
    width = target.shape[1]
    target[...] = source[:, span_of(info[CORE] * chips + info[CHIP], width)]


def keep_body(info, old, new, out, *, home):
    out[...] = jnp.where(info[SECTION] == home, new[...], old[...])


def join_body(info, *refs):
    assemble(info, refs[:-1], refs[-1])


def kv_body(info, *refs):
    pieces = refs[:-8]
    gain, w_kv, ahead, away, own, scale_out, gained, whole = refs[-8:]
    assemble(info, pieces, whole)
    scale = gain_rows(whole, gain, gained)
    projected = (dot(gained[...], w_kv[...]) * scale).astype(BF16)
    arranged = dot(projected, ahead[...]).astype(BF16)
    half = away.shape[1]
    away[...] = arranged[:, :half]
    own[...] = arranged[:, half:]
    scale_out[...] = jnp.broadcast_to(scale, scale_out.shape)


def merge_body(own, partner, *outs):
    span = own.shape[1]
    each = span // len(outs)
    row = lax.broadcasted_iota(jnp.int32, (span, 2 * each), 0)
    column = lax.broadcasted_iota(jnp.int32, (span, 2 * each), 1)
    for step, out in enumerate(outs):
        first = (row == column + step * each) & (column < each)
        second = (row == column + (step - 1) * each) & (column >= each)
        out[...] = (
            dot(own[...], first.astype(F32).astype(BF16))
            + dot(partner[...], second.astype(F32).astype(BF16))
        ).astype(BF16)


def query_body(gained, scale, w_query, queries):
    step = min(256, w_query.shape[1])
    for first in range(0, w_query.shape[1], step):
        at = slice(first, first + step)
        queries[:, at] = dot(gained[...], w_query[:, at]) * scale[:, :1]


def attend_body(info, codes, *refs, tick):
    arrived = refs[:-9]
    queries, after, cosine, sine, w_out, theirs, mine, context = refs[-9:-1]
    length = cosine.shape[0]
    batch = queries.shape[0] // length
    heads_here = queries.shape[1] // HD
    kv_here = after.shape[1] // (2 * HD)
    repeat_count = heads_here // kv_here
    cos = cosine[...]
    sin = sine[...]

    def turn(value):
        return (value * cos + pltpu.roll(value, HD // 2, 1) * sin).astype(BF16)

    row = lax.broadcasted_iota(jnp.int32, (length, length), 0)
    column = lax.broadcasted_iota(jnp.int32, (length, length), 1)
    wide = arrived[0].shape[1]
    for b in range(batch):
        rows = slice(b * length, (b + 1) * length)
        whole = dot(arrived[0][rows, :], after[:wide, :])
        for step in range(1, len(arrived)):
            whole = whole + dot(
                arrived[step][rows, :], after[step * wide : (step + 1) * wide, :]
            )
        for k in range(kv_here):
            keys = turn(whole[:, k * HD : (k + 1) * HD])
            at = (kv_here + k) * HD
            values = whole[:, at : at + HD].astype(BF16)
            for r in range(repeat_count):
                h = k * repeat_count + r
                lanes = slice(h * HD, (h + 1) * HD)
                query = turn(queries[rows, lanes])
                scores = lax.dot_general(
                    query, keys, (((1,), (1,)), ((), ())), preferred_element_type=F32
                ) * HD ** (-0.5)
                scores = jnp.where(row >= column, scores, -jnp.inf)
                weight = jnp.exp(scores - jnp.max(scores, axis=1, keepdims=True))
                weight = weight / jnp.sum(weight, axis=1, keepdims=True)
                mixed = dot(weight.astype(BF16), values)
                on = info[FIRST_HEAD] + h < codes[tick, b]
                context[rows, lanes] = jnp.where(on, mixed, 0.0).astype(BF16)
    halves_dot(info, context, w_out, theirs, mine, 512)


def ffn_body(info, codes, *refs, tick, batch):
    pieces = refs[:-8]
    inverse_gain, w_gate, w_up, w_down, theirs, mine, gained, hidden = refs[-8:]
    assemble(info, pieces, gained)
    scale = row_scale(gained, inverse_gain)
    step = 256
    rows = gained.shape[0]
    row = lax.broadcasted_iota(jnp.int32, (rows, step), 0)
    limit = jnp.full((rows, step), codes[tick, batch] * BLOCK - info[FIRST_UNIT], jnp.int32)
    for b in range(1, batch):
        here = codes[tick, batch + b] * BLOCK - info[FIRST_UNIT]
        limit = jnp.where(row >= b * (rows // batch), here, limit)

    for n in range(w_gate.shape[1] // step):
        at = slice(n * step, (n + 1) * step)
        gate = dot(gained[...], w_gate[:, at]) * scale
        up = dot(gained[...], w_up[:, at]) * scale
        unit = n * step + lax.broadcasted_iota(jnp.int32, gate.shape, 1)
        value = gate / (1.0 + jnp.exp(-gate)) * up
        hidden[:, at] = jnp.where(unit < limit, value, 0.0).astype(BF16)
    halves_dot(info, hidden, w_down, theirs, mine, 512)


def pair_body(info, mine, partner, own, *outs):
    width = own.shape[1]

    def summed(step):
        at = span_of(info[CHIP] ^ step, width)
        return mine[:, at].astype(F32) + partner[:, at].astype(F32)

    for step, out in enumerate(outs, 1):
        out[...] = summed(step).astype(BF16)
    own[...] = summed(0)


def finish_attention_body(*refs):
    part, own, gain = refs[:3]
    arrived, (attended, gained) = refs[3:-2], refs[-2:]
    total = own[...]
    for piece in arrived:
        total = total + piece[...].astype(F32)
    total = part[...].astype(F32) + total
    attended[...] = total
    gained[...] = (total * gain[...]).astype(BF16)


def finish_layer_body(*refs, last):
    attended, own = refs[:2]
    arrived, leaving = refs[2:-1], refs[-1]
    if last is not None:
        info, entering, *arrived = arrived
        *arrived, leaving = arrived + [leaving]
        *arrived, final = arrived
    total = own[...]
    for piece in arrived:
        total = total + piece[...].astype(F32)
    total = (attended[...] + total).astype(BF16)
    if last is None:
        leaving[...] = total
    else:
        final[...] = total
        leaving[...] = jnp.where(info[SECTION] == last, entering[...], total)


def exchange_tables(chip, core, chips, key_width, heads_here, kv_here):
    comps = key_width // KV_HEADS
    group = HEADS // KV_HEADS
    each = kv_here * 2 * comps
    out = jnp.arange(CORES * chips * each)
    own = out // (chips * each)
    step = out // each % chips
    dest = (chip ^ step) * CORES + jnp.where(own == 1, core, 1 - core)
    head = dest * heads_here // group + out // (2 * comps) % kv_here
    source = out // comps % 2 * key_width + out % comps * KV_HEADS + head
    ahead = (jnp.arange(2 * key_width)[:, None] == source[None, :]).astype(BF16)
    step = out // (CORES * each)
    other = out // each % CORES
    sender = (chip ^ step) * CORES + jnp.where(other == 1, 1 - core, core)
    head = out // (2 * comps) % kv_here
    target = out // comps % 2 * (kv_here * HD) + head * HD + sender * comps + out % comps
    after = (target[:, None] == jnp.arange(2 * kv_here * HD)[None, :]).astype(BF16)
    return ahead, after


def per_device(
    hidden_in,
    attn_gain,
    w_query,
    w_key,
    w_value,
    w_out,
    ffn_gain,
    w_gate,
    w_up,
    w_down,
    ffn_blocks,
    heads_on,
):
    sections = lax.axis_size("section")
    section = lax.axis_index("section")
    count = lax.axis_size("mp")
    chips = count // CORES
    index = lax.axis_index("mp")
    chip = index // CORES
    core = index % CORES
    per_section = hidden_in.shape[0]
    length = hidden_in.shape[2]
    model_width = hidden_in.shape[3]
    micro_total = ffn_blocks.shape[0]
    half_width = model_width // CORES
    width = model_width // count
    units_here = w_gate.shape[2]
    query_width = w_query.shape[2]
    key_width = w_key.shape[2]
    heads_here = query_width // HD
    kv_here = max(1, heads_here // (HEADS // KV_HEADS))
    each = kv_here * 2 * (key_width // KV_HEADS)
    span = chips * each
    rows = GROUP * length
    groups = micro_total // GROUP
    ticks = groups + sections - 1

    info = jnp.stack(
        [core, chip, section, index * heads_here, index * units_here]
    )
    first = jnp.clip(jnp.arange(ticks) - section, 0, groups - 1) * GROUP
    micro = first[:, None] + jnp.arange(GROUP)[None, :]
    pick = micro[:, :, None] == jnp.arange(micro_total)[None, None, :]
    codes = jnp.concatenate(
        [
            jnp.sum(jnp.where(pick, table[:, 0][None, None, :], 0), axis=2)
            for table in (heads_on, ffn_blocks)
        ],
        axis=1,
    )
    cosine, sine = rope_tables(length)
    ahead, after = exchange_tables(chip, core, chips, key_width, heads_here, kv_here)
    w_kv = jnp.concatenate([w_key[0], w_value[0]], axis=1)
    first_column = (core * chips + chip) * width
    gain_a = attn_gain[:1].astype(F32)
    gain_f = ffn_gain[:1].astype(F32)
    own_gain_f = lax.dynamic_slice_in_dim(gain_f, first_column, width, 1)
    inverse_f = 1.0 / gain_f

    small = (info, codes, cosine, sine, ahead, after, own_gain_f, gain_a, inverse_f)
    kv_w, query_w, out_w = resident((w_kv[None], w_query, w_out), small)
    gate_w, up_w, down_w = resident((w_gate, w_up, w_down), small)

    def to_core(array):
        return lax.ppermute(array, "mp", [(i, i ^ 1) for i in range(count)])

    def to_chip(array, step):
        return lax.ppermute(
            array, "mp", [(i, ((i // CORES) ^ step) * CORES + i % CORES) for i in range(count)]
        )

    def spread(piece):
        got = {step: to_chip(piece, step) for step in range(chips - 1, 0, -1)}
        got[0] = piece
        same = [got[step] for step in range(chips)]
        return same + [to_core(piece) for piece in same]

    def scatter(theirs, mine):
        partner = to_core(theirs)
        own, *away = kernel_call(
            pair_body,
            "pair_sum",
            [shaped(rows, width, F32)] + [shaped(rows, width)] * (chips - 1),
            [SMEM, VMEM, VMEM],
        )(info, mine, partner)
        return own, [to_chip(away[step - 1], step) for step in range(chips - 1, 0, -1)]

    half_out = [shaped(rows, half_width)] * CORES

    def layer(pieces, tick, entering):
        part = pieces[0]
        first_tick = tick == 0
        away, own, scale, whole = kernel_call(
            kv_body,
            "project_kv",
            [
                shaped(rows, span),
                shaped(rows, span),
                shaped(rows, LANES, F32),
                shaped(rows, model_width),
            ],
            [SMEM] + [VMEM] * (count + 3),
            [pltpu.VMEM((rows, model_width), BF16)],
        )(info, *pieces, gain_a, kv_w, ahead)
        partner = to_core(away)
        parts = kernel_call(
            merge_body, "merge_kv", [shaped(rows, CORES * each)] * chips, [VMEM, VMEM]
        )(own, partner)
        arrived = [parts[0]] + [to_chip(parts[step], step) for step in range(1, chips)]
        queries = kernel_call(
            query_body, "project_query", shaped(rows, query_width, F32), [VMEM] * 3
        )(whole, scale, query_w)

        early = []

        def attend(info, codes, *refs):
            attend_body(info, codes, *refs[len(early) :], None, tick=tick)

        theirs, mine = kernel_call(
            attend,
            "attend_out",
            half_out,
            [SMEM, SMEM] + [VMEM] * (chips + 5 + len(early)),
            [pltpu.VMEM((rows, query_width), BF16)],
        )(info, codes, *early, *arrived, queries, after, cosine, sine, out_w)
        own, arrived = scatter(theirs, mine)
        early = []

        def finish_attention(*refs):
            finish_attention_body(*refs[len(early) :])

        attended, gained = kernel_call(
            finish_attention,
            "finish_attention",
            [shaped(rows, width, F32), shaped(rows, width)],
            [VMEM] * (chips + 2 + len(early)),
        )(*early, part, own, own_gain_f, *arrived)

        def feed(*refs):
            ffn_body(*refs, tick=tick, batch=GROUP)

        theirs, mine = kernel_call(
            feed,
            "feed_forward",
            half_out,
            [SMEM, SMEM] + [VMEM] * (count + 4),
            [pltpu.VMEM((rows, model_width), BF16), pltpu.VMEM((rows, units_here), BF16)],
        )(info, codes, *spread(gained), inverse_f, gate_w, up_w, down_w)
        own, arrived = scatter(theirs, mine)
        if entering is None:

            def finish(*refs):
                finish_layer_body(*refs, last=None)

            leaving = kernel_call(
                finish, "finish_layer", shaped(rows, width), [VMEM] * (chips + 1)
            )(attended, own, *arrived)
            return leaving, leaving

        def finish(*refs):
            finish_layer_body(*refs, last=sections - 1)

        return kernel_call(
            finish,
            "finish_layer",
            [shaped(rows, width)] * 2,
            [VMEM, VMEM, SMEM] + [VMEM] * chips,
        )(attended, own, info, entering, *arrived)

    def cut(*refs):
        cut_body(*refs, chips=chips)

    own_input = [
        kernel_call(cut, "cut_input", shaped(length, width), [SMEM, VMEM])(
            info, hidden_in[cycle, 0]
        )
        for cycle in range(per_section)
    ]

    def brought(micro, to):
        cycle, home = divmod(micro, sections)
        if home == to:
            return own_input[cycle]
        return lax.ppermute(own_input[cycle], "section", [(home, to)])

    def stacked(blocks):
        return blocks[0] if len(blocks) == 1 else jnp.concatenate(blocks, axis=0)

    def entry(group, to):
        return stacked([brought(group * GROUP + k, to) for k in range(GROUP)])

    def handed_on(piece, around):
        same = []
        for step in range(chips):
            pairs = [
                (
                    s * count + i,
                    (s + 1) % sections * count + ((i // CORES) ^ step) * CORES + i % CORES,
                )
                for s in range(sections if around else sections - 1)
                for i in range(count)
            ]
            same.append(lax.ppermute(piece, ("section", "mp"), pairs))
        return same + [to_core(block) for block in same]

    entries = [entry(g, sections - 1 if g else 0) for g in range(groups)]
    pieces = spread(entries[0])
    finished = [None] * per_section
    for tick in range(ticks):
        enters = tick + 1 < groups
        final, leaving = layer(pieces, tick, entries[tick + 1] if enters else None)
        done = tick - (sections - 1)
        if done >= 0:
            for k in range(GROUP):
                cycle, home = divmod(done * GROUP + k, sections)
                block = final[k * length : (k + 1) * length]
                if home != sections - 1:
                    block = lax.ppermute(block, "section", [(sections - 1, home)])
                if finished[cycle] is None:
                    finished[cycle] = block
                else:

                    def keep(*refs, home=home):
                        keep_body(*refs, home=home)

                    finished[cycle] = kernel_call(
                        keep, "keep", shaped(length, width), [SMEM, VMEM, VMEM]
                    )(info, finished[cycle], block)
        if tick + 1 < ticks:
            pieces = handed_on(leaving, enters)
    results = [
        kernel_call(
            join_body, "join_output", shaped(length, model_width), [SMEM] + [VMEM] * count
        )(info, *spread(block))
        for block in finished
    ]
    return jnp.stack(results).reshape(hidden_in.shape)


def solution(mesh):
    return jax.shard_map(
        per_device,
        mesh=mesh,
        in_specs=(
            P(None, "section", None, None),
            P("section", None),
            P("section", None, "mp"),
            P("section", None, "mp"),
            P("section", None, "mp"),
            P("section", "mp", None),
            P("section", None),
            P("section", None, "mp"),
            P("section", None, "mp"),
            P("section", "mp", None),
            P(None, "section"),
            P(None, "section"),
        ),
        out_specs=P(None, "section", None, None),
        check_vma=False,
    )
```

```python
import jax
import jax.numpy as jnp
from jax import lax
from jax.experimental import pallas as pl
from jax.experimental.pallas import tpu as pltpu
from jax.sharding import PartitionSpec as P

HEADS = 32
KV_HEADS = 8
HD = 128
BLOCK = 128
CORES = 2
LANES = 128

ROPE_BASE = 500000.0
EPSILON = 1e-05
GROUP = 1


F32 = jnp.float32
BF16 = jnp.bfloat16

VMEM = pl.BlockSpec(memory_space=pltpu.VMEM)
SMEM = pl.BlockSpec(memory_space=pltpu.SMEM)
ANY = pl.BlockSpec(memory_space=pl.ANY)
CORE, CHIP, SECTION, FIRST_HEAD, FIRST_UNIT = range(5)


def dot(left, right):
    return jnp.dot(left, right, preferred_element_type=F32)


def shaped(rows, columns, dtype=BF16):
    return jax.ShapeDtypeStruct((rows, columns), dtype)


def kernel_call(body, name, out_shape, in_specs, scratch=()):
    many = isinstance(out_shape, (list, tuple))
    return pl.pallas_call(
        body,
        out_shape=out_shape,
        in_specs=in_specs,
        out_specs=[VMEM] * len(out_shape) if many else VMEM,
        scratch_shapes=list(scratch),
        compiler_params=pltpu.CompilerParams(vmem_limit_bytes=4 << 20),
        name=name,
    )


def rope_tables(length):
    half_dim = HD // 2
    frequency = ROPE_BASE ** (-(jnp.arange(half_dim, dtype=F32) / half_dim))
    angles = jnp.arange(length, dtype=F32)[:, None] * frequency[None, :]
    cosine = jnp.cos(angles)
    sine = jnp.sin(angles)
    return (
        jnp.concatenate([cosine, cosine], axis=1),
        jnp.concatenate([-sine, sine], axis=1),
    )


def span_of(index, width):
    return pl.ds(pl.multiple_of(index * width, width), width)


def assemble(info, pieces, whole):
    chips = len(pieces) // CORES
    width = pieces[0].shape[1]
    for core_step in range(CORES):
        for step in range(chips):
            core = info[CORE] ^ core_step
            block = core * chips + (info[CHIP] ^ step)
            whole[:, span_of(block, width)] = pieces[core_step * chips + step][...]


def gain_rows(rows, gain, gained):
    columns = rows.shape[1]
    total = jnp.zeros((rows.shape[0], LANES), F32)
    for first in range(0, columns, LANES):
        at = slice(first, first + LANES)
        value = rows[:, at].astype(F32)
        total = total + value * value
        gained[:, at] = (value * gain[:, at]).astype(BF16)
    mean_sq = jnp.sum(total, axis=1, keepdims=True) / columns
    return lax.rsqrt(mean_sq + EPSILON)


def row_scale(gained, inverse_gain):
    columns = gained.shape[1]
    total = jnp.zeros((gained.shape[0], LANES), F32)
    for first in range(0, columns, LANES):
        at = slice(first, first + LANES)
        value = gained[:, at].astype(F32) * inverse_gain[:, at]
        total = total + value * value
    mean_sq = jnp.sum(total, axis=1, keepdims=True) / columns
    return lax.rsqrt(mean_sq + EPSILON)


def halves_dot(info, left, weights, theirs, mine, step):
    half = theirs.shape[1]
    step = min(step, half)
    for out, core in ((theirs, 1 - info[CORE]), (mine, info[CORE])):
        for n in range(half // step):
            at = span_of(core * (half // step) + n, step)
            out[:, n * step : (n + 1) * step] = dot(left[...], weights[:, at]).astype(BF16)


def load_body(*refs, many):
    sources = refs[-3 * many : -2 * many]
    targets = refs[-2 * many : -many]
    copies = [
        pltpu.make_async_copy(source.at[0], target, arrived)
        for source, target, arrived in zip(sources, targets, refs[-many:])
    ]
    for copy in copies:
        copy.start()
    for copy in copies:
        copy.wait()


def resident(arrays, after):
    many = len(arrays)

    def load(*refs):
        load_body(*refs, many=many)

    return pl.pallas_call(
        load,
        out_shape=[pltpu.VMEM(array.shape[1:], array.dtype) for array in arrays],
        in_specs=[ANY] * len(after) + [pl.BlockSpec(memory_space=pltpu.HBM)] * many,
        out_specs=[VMEM] * many,
        scratch_shapes=[pltpu.SemaphoreType.DMA] * many,
        compiler_params=pltpu.CompilerParams(vmem_limit_bytes=1 << 18),
        name="resident",
    )(*after, *arrays)


def cut_body(info, anchor, source, target, *, chips):
    width = target.shape[1]
    target[...] = source[:, span_of(info[CORE] * chips + info[CHIP], width)]


def keep_body(info, old, new, out, *, home):
    out[...] = jnp.where(info[SECTION] == home, new[...], old[...])


def join_body(info, *refs):
    assemble(info, refs[:-1], refs[-1])


def kv_body(info, *refs):
    pieces = refs[:-8]
    gain, w_kv, ahead, away, own, scale_out, gained, whole = refs[-8:]
    assemble(info, pieces, whole)
    scale = gain_rows(whole, gain, gained)
    projected = (dot(gained[...], w_kv[...]) * scale).astype(BF16)
    arranged = dot(projected, ahead[...]).astype(BF16)
    half = away.shape[1]
    away[...] = arranged[:, :half]
    own[...] = arranged[:, half:]
    scale_out[...] = jnp.broadcast_to(scale, scale_out.shape)


def merge_body(own, partner, *outs):
    span = own.shape[1]
    each = span // len(outs)
    row = lax.broadcasted_iota(jnp.int32, (span, 2 * each), 0)
    column = lax.broadcasted_iota(jnp.int32, (span, 2 * each), 1)
    for step, out in enumerate(outs):
        first = (row == column + step * each) & (column < each)
        second = (row == column + (step - 1) * each) & (column >= each)
        out[...] = (
            dot(own[...], first.astype(F32).astype(BF16))
            + dot(partner[...], second.astype(F32).astype(BF16))
        ).astype(BF16)


def query_body(gained, scale, w_query, queries):
    step = min(256, w_query.shape[1])
    for first in range(0, w_query.shape[1], step):
        at = slice(first, first + step)
        queries[:, at] = dot(gained[...], w_query[:, at]) * scale[:, :1]


def attend_body(info, codes, *refs, tick):
    arrived = refs[:-9]
    queries, after, cosine, sine, w_out, theirs, mine, context = refs[-9:-1]
    length = cosine.shape[0]
    batch = queries.shape[0] // length
    heads_here = queries.shape[1] // HD
    kv_here = after.shape[1] // (2 * HD)
    repeat_count = heads_here // kv_here
    cos = cosine[...]
    sin = sine[...]

    def turn(value):
        return (value * cos + pltpu.roll(value, HD // 2, 1) * sin).astype(BF16)

    row = lax.broadcasted_iota(jnp.int32, (length, length), 0)
    column = lax.broadcasted_iota(jnp.int32, (length, length), 1)
    wide = arrived[0].shape[1]
    for b in range(batch):
        rows = slice(b * length, (b + 1) * length)
        whole = dot(arrived[0][rows, :], after[:wide, :])
        for step in range(1, len(arrived)):
            whole = whole + dot(
                arrived[step][rows, :], after[step * wide : (step + 1) * wide, :]
            )
        for k in range(kv_here):
            keys = turn(whole[:, k * HD : (k + 1) * HD])
            at = (kv_here + k) * HD
            values = whole[:, at : at + HD].astype(BF16)
            for r in range(repeat_count):
                h = k * repeat_count + r
                lanes = slice(h * HD, (h + 1) * HD)
                query = turn(queries[rows, lanes])
                scores = lax.dot_general(
                    query, keys, (((1,), (1,)), ((), ())), preferred_element_type=F32
                ) * HD ** (-0.5)
                scores = jnp.where(row >= column, scores, -jnp.inf)
                weight = jnp.exp(scores - jnp.max(scores, axis=1, keepdims=True))
                weight = weight / jnp.sum(weight, axis=1, keepdims=True)
                mixed = dot(weight.astype(BF16), values)
                on = info[FIRST_HEAD] + h < codes[tick, b]
                context[rows, lanes] = jnp.where(on, mixed, 0.0).astype(BF16)
    halves_dot(info, context, w_out, theirs, mine, 512)


def ffn_body(info, codes, *refs, tick, batch):
    pieces = refs[:-8]
    inverse_gain, w_gate, w_up, w_down, theirs, mine, gained, hidden = refs[-8:]
    assemble(info, pieces, gained)
    scale = row_scale(gained, inverse_gain)
    step = 256
    rows = gained.shape[0]
    row = lax.broadcasted_iota(jnp.int32, (rows, step), 0)
    limit = jnp.full((rows, step), codes[tick, batch] * BLOCK - info[FIRST_UNIT], jnp.int32)
    for b in range(1, batch):
        here = codes[tick, batch + b] * BLOCK - info[FIRST_UNIT]
        limit = jnp.where(row >= b * (rows // batch), here, limit)

    for n in range(w_gate.shape[1] // step):
        at = slice(n * step, (n + 1) * step)
        gate = dot(gained[...], w_gate[:, at]) * scale
        up = dot(gained[...], w_up[:, at]) * scale
        unit = n * step + lax.broadcasted_iota(jnp.int32, gate.shape, 1)
        value = gate / (1.0 + jnp.exp(-gate)) * up
        hidden[:, at] = jnp.where(unit < limit, value, 0.0).astype(BF16)
    halves_dot(info, hidden, w_down, theirs, mine, 512)


def pair_body(info, mine, partner, own, *outs):
    width = own.shape[1]

    def summed(step):
        at = span_of(info[CHIP] ^ step, width)
        return mine[:, at].astype(F32) + partner[:, at].astype(F32)

    for step, out in enumerate(outs, 1):
        out[...] = summed(step).astype(BF16)
    own[...] = summed(0)


def finish_attention_body(*refs):
    part, own, gain = refs[:3]
    arrived, (attended, gained) = refs[3:-2], refs[-2:]
    total = own[...]
    for piece in arrived:
        total = total + piece[...].astype(F32)
    total = part[...].astype(F32) + total
    attended[...] = total
    gained[...] = (total * gain[...]).astype(BF16)


def finish_layer_body(*refs, last):
    attended, own = refs[:2]
    arrived, leaving = refs[2:-1], refs[-1]
    if last is not None:
        info, entering, *arrived = arrived
        *arrived, leaving = arrived + [leaving]
        *arrived, final = arrived
    total = own[...]
    for piece in arrived:
        total = total + piece[...].astype(F32)
    total = (attended[...] + total).astype(BF16)
    if last is None:
        leaving[...] = total
    else:
        final[...] = total
        leaving[...] = jnp.where(info[SECTION] == last, entering[...], total)


def exchange_tables(chip, core, chips, key_width, heads_here, kv_here):
    comps = key_width // KV_HEADS
    group = HEADS // KV_HEADS
    each = kv_here * 2 * comps
    out = jnp.arange(CORES * chips * each)
    own = out // (chips * each)
    step = out // each % chips
    dest = (chip ^ step) * CORES + jnp.where(own == 1, core, 1 - core)
    head = dest * heads_here // group + out // (2 * comps) % kv_here
    source = out // comps % 2 * key_width + out % comps * KV_HEADS + head
    ahead = (jnp.arange(2 * key_width)[:, None] == source[None, :]).astype(BF16)
    step = out // (CORES * each)
    other = out // each % CORES
    sender = (chip ^ step) * CORES + jnp.where(other == 1, 1 - core, core)
    head = out // (2 * comps) % kv_here
    target = out // comps % 2 * (kv_here * HD) + head * HD + sender * comps + out % comps
    after = (target[:, None] == jnp.arange(2 * kv_here * HD)[None, :]).astype(BF16)
    return ahead, after


def per_device(
    hidden_in,
    attn_gain,
    w_query,
    w_key,
    w_value,
    w_out,
    ffn_gain,
    w_gate,
    w_up,
    w_down,
    ffn_blocks,
    heads_on,
):
    sections = lax.axis_size("section")
    section = lax.axis_index("section")
    count = lax.axis_size("mp")
    chips = count // CORES
    index = lax.axis_index("mp")
    chip = index // CORES
    core = index % CORES
    per_section = hidden_in.shape[0]
    length = hidden_in.shape[2]
    model_width = hidden_in.shape[3]
    micro_total = ffn_blocks.shape[0]
    half_width = model_width // CORES
    width = model_width // count
    units_here = w_gate.shape[2]
    query_width = w_query.shape[2]
    key_width = w_key.shape[2]
    heads_here = query_width // HD
    kv_here = max(1, heads_here // (HEADS // KV_HEADS))
    each = kv_here * 2 * (key_width // KV_HEADS)
    span = chips * each
    rows = GROUP * length
    groups = micro_total // GROUP
    ticks = groups + sections - 1

    info = jnp.stack(
        [core, chip, section, index * heads_here, index * units_here]
    )
    first = jnp.clip(jnp.arange(ticks) - section, 0, groups - 1) * GROUP
    micro = first[:, None] + jnp.arange(GROUP)[None, :]
    pick = micro[:, :, None] == jnp.arange(micro_total)[None, None, :]
    codes = jnp.concatenate(
        [
            jnp.sum(jnp.where(pick, table[:, 0][None, None, :], 0), axis=2)
            for table in (heads_on, ffn_blocks)
        ],
        axis=1,
    )
    cosine, sine = rope_tables(length)
    ahead, after = exchange_tables(chip, core, chips, key_width, heads_here, kv_here)
    w_kv = jnp.concatenate([w_key[0], w_value[0]], axis=1)
    first_column = (core * chips + chip) * width
    gain_a = attn_gain[:1].astype(F32)
    gain_f = ffn_gain[:1].astype(F32)
    own_gain_f = lax.dynamic_slice_in_dim(gain_f, first_column, width, 1)
    inverse_f = 1.0 / gain_f

    small = (info, codes, cosine, sine, ahead, after, own_gain_f, gain_a, inverse_f)
    (kv_w,) = resident((w_kv[None],), small)
    (query_w,) = resident((w_query,), small)
    (out_w,) = resident((w_out,), small)
    (gate_w,) = resident((w_gate,), small)
    (up_w,) = resident((w_up,), small)
    (down_w,) = resident((w_down,), small)

    def to_core(array):
        return lax.ppermute(array, "mp", [(i, i ^ 1) for i in range(count)])

    def to_chip(array, step):
        return lax.ppermute(
            array, "mp", [(i, ((i // CORES) ^ step) * CORES + i % CORES) for i in range(count)]
        )

    def spread(piece):
        got = {step: to_chip(piece, step) for step in range(chips - 1, 0, -1)}
        got[0] = piece
        same = [got[step] for step in range(chips)]
        return same + [to_core(piece) for piece in same]

    def scatter(theirs, mine):
        partner = to_core(theirs)
        own, *away = kernel_call(
            pair_body,
            "pair_sum",
            [shaped(rows, width, F32)] + [shaped(rows, width)] * (chips - 1),
            [SMEM, VMEM, VMEM],
        )(info, mine, partner)
        return own, [to_chip(away[step - 1], step) for step in range(chips - 1, 0, -1)]

    half_out = [shaped(rows, half_width)] * CORES

    def layer(pieces, tick, entering):
        part = pieces[0]
        first_tick = tick == 0
        away, own, scale, whole = kernel_call(
            kv_body,
            "project_kv",
            [
                shaped(rows, span),
                shaped(rows, span),
                shaped(rows, LANES, F32),
                shaped(rows, model_width),
            ],
            [SMEM] + [VMEM] * (count + 3),
            [pltpu.VMEM((rows, model_width), BF16)],
        )(info, *pieces, gain_a, kv_w, ahead)
        partner = to_core(away)
        parts = kernel_call(
            merge_body, "merge_kv", [shaped(rows, CORES * each)] * chips, [VMEM, VMEM]
        )(own, partner)
        arrived = [parts[0]] + [to_chip(parts[step], step) for step in range(1, chips)]
        queries = kernel_call(
            query_body, "project_query", shaped(rows, query_width, F32), [VMEM] * 3
        )(whole, scale, query_w)

        early = []

        def attend(info, codes, *refs):
            attend_body(info, codes, *refs[len(early) :], None, tick=tick)

        theirs, mine = kernel_call(
            attend,
            "attend_out",
            half_out,
            [SMEM, SMEM] + [VMEM] * (chips + 5 + len(early)),
            [pltpu.VMEM((rows, query_width), BF16)],
        )(info, codes, *early, *arrived, queries, after, cosine, sine, out_w)
        own, arrived = scatter(theirs, mine)
        early = []

        def finish_attention(*refs):
            finish_attention_body(*refs[len(early) :])

        attended, gained = kernel_call(
            finish_attention,
            "finish_attention",
            [shaped(rows, width, F32), shaped(rows, width)],
            [VMEM] * (chips + 2 + len(early)),
        )(*early, part, own, own_gain_f, *arrived)

        def feed(*refs):
            ffn_body(*refs, tick=tick, batch=GROUP)

        theirs, mine = kernel_call(
            feed,
            "feed_forward",
            half_out,
            [SMEM, SMEM] + [VMEM] * (count + 4),
            [pltpu.VMEM((rows, model_width), BF16), pltpu.VMEM((rows, units_here), BF16)],
        )(info, codes, *spread(gained), inverse_f, gate_w, up_w, down_w)
        own, arrived = scatter(theirs, mine)
        if entering is None:

            def finish(*refs):
                finish_layer_body(*refs, last=None)

            leaving = kernel_call(
                finish, "finish_layer", shaped(rows, width), [VMEM] * (chips + 1)
            )(attended, own, *arrived)
            return leaving, leaving

        def finish(*refs):
            finish_layer_body(*refs, last=sections - 1)

        return kernel_call(
            finish,
            "finish_layer",
            [shaped(rows, width)] * 2,
            [VMEM, VMEM, SMEM] + [VMEM] * chips,
        )(attended, own, info, entering, *arrived)

    def cut(*refs):
        cut_body(*refs, chips=chips)

    def brought(micro, to, anchor):
        cycle, home = divmod(micro, sections)
        block = kernel_call(cut, "cut_input", shaped(length, width), [SMEM, ANY, VMEM])(
            info, anchor, hidden_in[cycle, 0]
        )
        if home == to:
            return block
        return lax.ppermute(block, "section", [(home, to)])

    def stacked(blocks):
        return blocks[0] if len(blocks) == 1 else jnp.concatenate(blocks, axis=0)

    def entry(group, to, anchor):
        return stacked([brought(group * GROUP + k, to, anchor) for k in range(GROUP)])

    def handed_on(piece, around):
        same = []
        for step in range(chips):
            pairs = [
                (
                    s * count + i,
                    (s + 1) % sections * count + ((i // CORES) ^ step) * CORES + i % CORES,
                )
                for s in range(sections if around else sections - 1)
                for i in range(count)
            ]
            same.append(lax.ppermute(piece, ("section", "mp"), pairs))
        return same + [to_core(block) for block in same]

    pieces = spread(entry(0, 0, info))
    finished = [None] * per_section
    for tick in range(ticks):
        enters = tick + 1 < groups
        entering = entry(tick + 1, sections - 1, pieces[-1]) if enters else None
        final, leaving = layer(pieces, tick, entering)
        done = tick - (sections - 1)
        if done >= 0:
            for k in range(GROUP):
                cycle, home = divmod(done * GROUP + k, sections)
                block = final[k * length : (k + 1) * length]
                if home != sections - 1:
                    block = lax.ppermute(block, "section", [(sections - 1, home)])
                if finished[cycle] is None:
                    finished[cycle] = block
                else:

                    def keep(*refs, home=home):
                        keep_body(*refs, home=home)

                    finished[cycle] = kernel_call(
                        keep, "keep", shaped(length, width), [SMEM, VMEM, VMEM]
                    )(info, finished[cycle], block)
        if tick + 1 < ticks:
            pieces = handed_on(leaving, enters)
    results = [
        kernel_call(
            join_body, "join_output", shaped(length, model_width), [SMEM] + [VMEM] * count
        )(info, *spread(block))
        for block in finished
    ]
    return jnp.stack(results).reshape(hidden_in.shape)


def solution(mesh):
    return jax.shard_map(
        per_device,
        mesh=mesh,
        in_specs=(
            P(None, "section", None, None),
            P("section", None),
            P("section", None, "mp"),
            P("section", None, "mp"),
            P("section", None, "mp"),
            P("section", "mp", None),
            P("section", None),
            P("section", None, "mp"),
            P("section", None, "mp"),
            P("section", "mp", None),
            P(None, "section"),
            P(None, "section"),
        ),
        out_specs=P(None, "section", None, None),
        check_vma=False,
    )
```

```python
import jax
import jax.numpy as jnp
from jax import lax
from jax.experimental import pallas as pl
from jax.experimental.pallas import tpu as pltpu
from jax.sharding import PartitionSpec as P

HEADS = 32
KV_HEADS = 8
HD = 128
BLOCK = 128
CORES = 2
LANES = 128

ROPE_BASE = 500000.0
EPSILON = 1e-05
GROUP = 1


F32 = jnp.float32
BF16 = jnp.bfloat16

VMEM = pl.BlockSpec(memory_space=pltpu.VMEM)
ANY = pl.BlockSpec(memory_space=pl.ANY)
WIDE = 256
CORE, CHIP = range(2)


def dot(left, right):
    return jnp.dot(left, right, preferred_element_type=F32)


def shaped(rows, columns, dtype=BF16):
    return jax.ShapeDtypeStruct((rows, columns), dtype)


def kernel_call(body, name, out_shape, in_specs, scratch=()):
    many = isinstance(out_shape, (list, tuple))
    return pl.pallas_call(
        body,
        out_shape=out_shape,
        in_specs=in_specs,
        out_specs=[VMEM] * len(out_shape) if many else VMEM,
        scratch_shapes=list(scratch),
        compiler_params=pltpu.CompilerParams(vmem_limit_bytes=4 << 20),
        name=name,
    )


def rope_tables(length):
    half_dim = HD // 2
    frequency = ROPE_BASE ** (-(jnp.arange(half_dim, dtype=F32) / half_dim))
    angles = jnp.arange(length, dtype=F32)[:, None] * frequency[None, :]
    cosine = jnp.cos(angles)
    sine = jnp.sin(angles)
    return (
        jnp.concatenate([cosine, cosine], axis=1),
        jnp.concatenate([-sine, sine], axis=1),
    )


def here():
    index = lax.axis_index("mp")
    return index % CORES, index // CORES


def span_of(index, width):
    return pl.ds(pl.multiple_of(index * width, width), width)


def assemble(pieces, whole):
    info = here()
    chips = len(pieces) // CORES
    width = pieces[0].shape[1]
    for core_step in range(CORES):
        for step in range(chips):
            core = info[CORE] ^ core_step
            block = core * chips + (info[CHIP] ^ step)
            whole[:, span_of(block, width)] = pieces[core_step * chips + step][...]


def gain_rows(rows, gain, gained):
    columns = rows.shape[1]
    total = jnp.zeros((rows.shape[0], LANES), F32)
    for first in range(0, columns, LANES):
        at = slice(first, first + LANES)
        value = rows[:, at].astype(F32)
        total = total + value * value
        gained[:, at] = (value * gain[:, at]).astype(BF16)
    mean_sq = jnp.sum(total, axis=1, keepdims=True) / columns
    return lax.rsqrt(mean_sq + EPSILON)


def row_scale(gained, inverse_gain):
    columns = gained.shape[1]
    total = jnp.zeros((gained.shape[0], LANES), F32)
    for first in range(0, columns, LANES):
        at = slice(first, first + LANES)
        value = gained[:, at].astype(F32) * inverse_gain[:, at]
        total = total + value * value
    mean_sq = jnp.sum(total, axis=1, keepdims=True) / columns
    return lax.rsqrt(mean_sq + EPSILON)


def halves_dot(left, weights, theirs, mine, step):
    info = here()
    half = theirs.shape[1]
    step = min(step, half)
    for out, core in ((theirs, 1 - info[CORE]), (mine, info[CORE])):
        for n in range(half // step):
            at = span_of(core * (half // step) + n, step)
            out[:, n * step : (n + 1) * step] = dot(left[...], weights[:, at]).astype(BF16)


def load_body(*refs, many):
    sources = refs[-3 * many : -2 * many]
    targets = refs[-2 * many : -many]
    copies = [
        pltpu.make_async_copy(source.at[0], target, arrived)
        for source, target, arrived in zip(sources, targets, refs[-many:])
    ]
    for copy in copies:
        copy.start()
    for copy in copies:
        copy.wait()


def resident(arrays, after):
    many = len(arrays)

    def load(*refs):
        load_body(*refs, many=many)

    return pl.pallas_call(
        load,
        out_shape=[pltpu.VMEM(array.shape[1:], array.dtype) for array in arrays],
        in_specs=[ANY] * len(after) + [pl.BlockSpec(memory_space=pltpu.HBM)] * many,
        out_specs=[VMEM] * many,
        scratch_shapes=[pltpu.SemaphoreType.DMA] * many,
        compiler_params=pltpu.CompilerParams(vmem_limit_bytes=1 << 18),
        name="resident",
    )(*after, *arrays)


def cut_body(anchor, source, target, *, chips):
    info = here()
    width = target.shape[1]
    target[...] = source[:, span_of(info[CORE] * chips + info[CHIP], width)]


def keep_body(old, new, out, *, home):
    out[...] = jnp.where(lax.axis_index("section") == home, new[...], old[...])


def join_body(*refs):
    assemble(refs[:-1], refs[-1])


def kv_body(*refs):
    pieces = refs[:-8]
    gain, w_kv, ahead, away, own, scale_out, gained, whole = refs[-8:]
    assemble(pieces, whole)
    scale = gain_rows(whole, gain, gained)
    projected = (dot(gained[...], w_kv[...]) * scale).astype(BF16)
    arranged = dot(projected, ahead[...]).astype(BF16)
    half = away.shape[1]
    away[...] = arranged[:, :half]
    own[...] = arranged[:, half:]
    scale_out[...] = jnp.broadcast_to(scale, scale_out.shape)


def merge_body(own, partner, *outs):
    span = own.shape[1]
    each = span // len(outs)
    row = lax.broadcasted_iota(jnp.int32, (span, 2 * each), 0)
    column = lax.broadcasted_iota(jnp.int32, (span, 2 * each), 1)
    for step, out in enumerate(outs):
        first = (row == column + step * each) & (column < each)
        second = (row == column + (step - 1) * each) & (column >= each)
        out[...] = (
            dot(own[...], first.astype(F32).astype(BF16))
            + dot(partner[...], second.astype(F32).astype(BF16))
        ).astype(BF16)


def query_body(gained, scale, w_query, queries):
    step = min(256, w_query.shape[1])
    for first in range(0, w_query.shape[1], step):
        at = slice(first, first + step)
        queries[:, at] = dot(gained[...], w_query[:, at]) * scale[:, :1]


def attend_body(codes, *refs, tick):
    arrived = refs[:-9]
    queries, after, cosine, sine, w_out, theirs, mine, context = refs[-9:-1]
    length = cosine.shape[0]
    batch = queries.shape[0] // length
    heads_here = queries.shape[1] // HD
    first_head = lax.axis_index("mp") * heads_here
    kv_here = after.shape[1] // (2 * HD)
    repeat_count = heads_here // kv_here
    cos = cosine[...]
    sin = sine[...]

    def turn(value):
        return (value * cos + pltpu.roll(value, HD // 2, 1) * sin).astype(BF16)

    row = lax.broadcasted_iota(jnp.int32, (length, length), 0)
    column = lax.broadcasted_iota(jnp.int32, (length, length), 1)
    wide = arrived[0].shape[1]
    for b in range(batch):
        rows = slice(b * length, (b + 1) * length)
        whole = dot(arrived[0][rows, :], after[:wide, :])
        for step in range(1, len(arrived)):
            whole = whole + dot(
                arrived[step][rows, :], after[step * wide : (step + 1) * wide, :]
            )
        for k in range(kv_here):
            keys = turn(whole[:, k * HD : (k + 1) * HD])
            at = (kv_here + k) * HD
            values = whole[:, at : at + HD].astype(BF16)
            for r in range(repeat_count):
                h = k * repeat_count + r
                lanes = slice(h * HD, (h + 1) * HD)
                query = turn(queries[rows, lanes])
                scores = lax.dot_general(
                    query, keys, (((1,), (1,)), ((), ())), preferred_element_type=F32
                ) * HD ** (-0.5)
                scores = jnp.where(row >= column, scores, -jnp.inf)
                weight = jnp.exp(scores - jnp.max(scores, axis=1, keepdims=True))
                weight = weight / jnp.sum(weight, axis=1, keepdims=True)
                mixed = dot(weight.astype(BF16), values)
                line = tick * 2 * batch + b
                on = first_head + h < codes[line : line + 1, :HD]
                context[rows, lanes] = jnp.where(on, mixed, 0.0).astype(BF16)
    halves_dot(context, w_out, theirs, mine, 512)


def ffn_body(codes, *refs, tick, batch):
    pieces = refs[:-8]
    inverse_gain, w_gate, w_up, w_down, theirs, mine, gained, hidden = refs[-8:]
    assemble(pieces, gained)
    scale = row_scale(gained, inverse_gain)
    step = WIDE
    rows = gained.shape[0]
    row = lax.broadcasted_iota(jnp.int32, (rows, step), 0)
    first_unit = lax.axis_index("mp") * w_gate.shape[1]
    line = (tick * 2 + 1) * batch
    limit = codes[line : line + 1, :] * BLOCK - first_unit
    for b in range(1, batch):
        later = codes[line + b : line + b + 1, :] * BLOCK - first_unit
        limit = jnp.where(row >= b * (rows // batch), later, limit)

    for n in range(w_gate.shape[1] // step):
        at = slice(n * step, (n + 1) * step)
        gate = dot(gained[...], w_gate[:, at]) * scale
        up = dot(gained[...], w_up[:, at]) * scale
        unit = n * step + lax.broadcasted_iota(jnp.int32, gate.shape, 1)
        value = gate / (1.0 + jnp.exp(-gate)) * up
        hidden[:, at] = jnp.where(unit < limit, value, 0.0).astype(BF16)
    halves_dot(hidden, w_down, theirs, mine, 512)


def pair_body(mine, partner, own, *outs):
    info = here()
    width = own.shape[1]

    def summed(step):
        at = span_of(info[CHIP] ^ step, width)
        return mine[:, at].astype(F32) + partner[:, at].astype(F32)

    for step, out in enumerate(outs, 1):
        out[...] = summed(step).astype(BF16)
    own[...] = summed(0)


def finish_attention_body(*refs):
    part, own, gain = refs[:3]
    arrived, (attended, gained) = refs[3:-2], refs[-2:]
    total = own[...]
    for piece in arrived:
        total = total + piece[...].astype(F32)
    total = part[...].astype(F32) + total
    attended[...] = total
    gained[...] = (total * gain[...]).astype(BF16)


def finish_layer_body(*refs, last):
    attended, own = refs[:2]
    arrived, leaving = refs[2:-1], refs[-1]
    if last is not None:
        entering, *arrived = arrived
        *arrived, leaving = arrived + [leaving]
        *arrived, final = arrived
    total = own[...]
    for piece in arrived:
        total = total + piece[...].astype(F32)
    total = (attended[...] + total).astype(BF16)
    if last is None:
        leaving[...] = total
    else:
        final[...] = total
        leaving[...] = jnp.where(
            lax.axis_index("section") == last, entering[...], total
        )


def exchange_tables(chip, core, chips, key_width, heads_here, kv_here):
    comps = key_width // KV_HEADS
    group = HEADS // KV_HEADS
    each = kv_here * 2 * comps
    out = jnp.arange(CORES * chips * each)
    own = out // (chips * each)
    step = out // each % chips
    dest = (chip ^ step) * CORES + jnp.where(own == 1, core, 1 - core)
    head = dest * heads_here // group + out // (2 * comps) % kv_here
    source = out // comps % 2 * key_width + out % comps * KV_HEADS + head
    ahead = (jnp.arange(2 * key_width)[:, None] == source[None, :]).astype(BF16)
    step = out // (CORES * each)
    other = out // each % CORES
    sender = (chip ^ step) * CORES + jnp.where(other == 1, 1 - core, core)
    head = out // (2 * comps) % kv_here
    target = out // comps % 2 * (kv_here * HD) + head * HD + sender * comps + out % comps
    after = (target[:, None] == jnp.arange(2 * kv_here * HD)[None, :]).astype(BF16)
    return ahead, after


def per_device(
    hidden_in,
    attn_gain,
    w_query,
    w_key,
    w_value,
    w_out,
    ffn_gain,
    w_gate,
    w_up,
    w_down,
    ffn_blocks,
    heads_on,
):
    sections = lax.axis_size("section")
    section = lax.axis_index("section")
    count = lax.axis_size("mp")
    chips = count // CORES
    index = lax.axis_index("mp")
    chip = index // CORES
    core = index % CORES
    per_section = hidden_in.shape[0]
    length = hidden_in.shape[2]
    model_width = hidden_in.shape[3]
    micro_total = ffn_blocks.shape[0]
    half_width = model_width // CORES
    width = model_width // count
    units_here = w_gate.shape[2]
    query_width = w_query.shape[2]
    key_width = w_key.shape[2]
    heads_here = query_width // HD
    kv_here = max(1, heads_here // (HEADS // KV_HEADS))
    each = kv_here * 2 * (key_width // KV_HEADS)
    span = chips * each
    rows = GROUP * length
    groups = micro_total // GROUP
    ticks = groups + sections - 1

    first = jnp.clip(jnp.arange(ticks) - section, 0, groups - 1) * GROUP
    micro = first[:, None] + jnp.arange(GROUP)[None, :]
    pick = micro[:, :, None] == jnp.arange(micro_total)[None, None, :]
    codes = jnp.concatenate(
        [
            jnp.sum(jnp.where(pick, table[:, 0][None, None, :], 0), axis=2)
            for table in (heads_on, ffn_blocks)
        ],
        axis=1,
    )
    codes = jnp.broadcast_to(codes.reshape(-1, 1), (codes.size, WIDE))
    cosine, sine = rope_tables(length)
    ahead, after = exchange_tables(chip, core, chips, key_width, heads_here, kv_here)
    w_kv = jnp.concatenate([w_key[0], w_value[0]], axis=1)
    first_column = (core * chips + chip) * width
    gain_a = attn_gain[:1].astype(F32)
    gain_f = ffn_gain[:1].astype(F32)
    own_gain_f = lax.dynamic_slice_in_dim(gain_f, first_column, width, 1)
    inverse_f = 1.0 / gain_f

    small = (codes, cosine, sine, ahead, after, own_gain_f, gain_a, inverse_f)
    (kv_w,) = resident((w_kv[None],), small)
    (query_w,) = resident((w_query,), small)
    (out_w,) = resident((w_out,), small)
    (gate_w,) = resident((w_gate,), small)
    (up_w,) = resident((w_up,), small)
    (down_w,) = resident((w_down,), small)

    def to_core(array):
        return lax.ppermute(array, "mp", [(i, i ^ 1) for i in range(count)])

    def to_chip(array, step):
        return lax.ppermute(
            array, "mp", [(i, ((i // CORES) ^ step) * CORES + i % CORES) for i in range(count)]
        )

    def spread(piece):
        got = {step: to_chip(piece, step) for step in range(chips - 1, 0, -1)}
        got[0] = piece
        same = [got[step] for step in range(chips)]
        return same + [to_core(piece) for piece in same]

    def scatter(theirs, mine):
        partner = to_core(theirs)
        own, *away = kernel_call(
            pair_body,
            "pair_sum",
            [shaped(rows, width, F32)] + [shaped(rows, width)] * (chips - 1),
            [VMEM, VMEM],
        )(mine, partner)
        return own, [to_chip(away[step - 1], step) for step in range(chips - 1, 0, -1)]

    half_out = [shaped(rows, half_width)] * CORES

    def layer(pieces, tick, entering):
        part = pieces[0]
        away, own, scale, whole = kernel_call(
            kv_body,
            "project_kv",
            [
                shaped(rows, span),
                shaped(rows, span),
                shaped(rows, LANES, F32),
                shaped(rows, model_width),
            ],
            [VMEM] * (count + 3),
            [pltpu.VMEM((rows, model_width), BF16)],
        )(*pieces, gain_a, kv_w, ahead)
        partner = to_core(away)
        parts = kernel_call(
            merge_body, "merge_kv", [shaped(rows, CORES * each)] * chips, [VMEM, VMEM]
        )(own, partner)
        arrived = [parts[0]] + [to_chip(parts[step], step) for step in range(1, chips)]
        queries = kernel_call(
            query_body, "project_query", shaped(rows, query_width, F32), [VMEM] * 3
        )(whole, scale, query_w)

        def attend(codes, *refs):
            attend_body(codes, *refs, None, tick=tick)

        theirs, mine = kernel_call(
            attend,
            "attend_out",
            half_out,
            [VMEM] * (chips + 6),
            [pltpu.VMEM((rows, query_width), BF16)],
        )(codes, *arrived, queries, after, cosine, sine, out_w)
        own, arrived = scatter(theirs, mine)
        attended, gained = kernel_call(
            finish_attention_body,
            "finish_attention",
            [shaped(rows, width, F32), shaped(rows, width)],
            [VMEM] * (chips + 2),
        )(part, own, own_gain_f, *arrived)

        def feed(*refs):
            ffn_body(*refs, tick=tick, batch=GROUP)

        theirs, mine = kernel_call(
            feed,
            "feed_forward",
            half_out,
            [VMEM] * (count + 5),
            [pltpu.VMEM((rows, model_width), BF16), pltpu.VMEM((rows, units_here), BF16)],
        )(codes, *spread(gained), inverse_f, gate_w, up_w, down_w)
        own, arrived = scatter(theirs, mine)
        if entering is None:

            def finish(*refs):
                finish_layer_body(*refs, last=None)

            leaving = kernel_call(
                finish, "finish_layer", shaped(rows, width), [VMEM] * (chips + 1)
            )(attended, own, *arrived)
            return leaving, leaving

        def finish(*refs):
            finish_layer_body(*refs, last=sections - 1)

        return kernel_call(
            finish,
            "finish_layer",
            [shaped(rows, width)] * 2,
            [VMEM] * (chips + 2),
        )(attended, own, entering, *arrived)

    def cut(*refs):
        cut_body(*refs, chips=chips)

    def brought(micro, to, anchor):
        cycle, home = divmod(micro, sections)
        block = kernel_call(cut, "cut_input", shaped(length, width), [ANY, VMEM])(
            anchor, hidden_in[cycle, 0]
        )
        if home == to:
            return block
        return lax.ppermute(block, "section", [(home, to)])

    def stacked(blocks):
        return blocks[0] if len(blocks) == 1 else jnp.concatenate(blocks, axis=0)

    def entry(group, to, anchor):
        return stacked([brought(group * GROUP + k, to, anchor) for k in range(GROUP)])

    def handed_on(piece, around):
        same = []
        for step in range(chips):
            pairs = [
                (
                    s * count + i,
                    (s + 1) % sections * count + ((i // CORES) ^ step) * CORES + i % CORES,
                )
                for s in range(sections if around else sections - 1)
                for i in range(count)
            ]
            same.append(lax.ppermute(piece, ("section", "mp"), pairs))
        return same + [to_core(block) for block in same]

    pieces = spread(entry(0, 0, codes))
    finished = [None] * per_section
    for tick in range(ticks):
        enters = tick + 1 < groups
        entering = entry(tick + 1, sections - 1, pieces[-1]) if enters else None
        final, leaving = layer(pieces, tick, entering)
        done = tick - (sections - 1)
        if done >= 0:
            for k in range(GROUP):
                cycle, home = divmod(done * GROUP + k, sections)
                block = final[k * length : (k + 1) * length]
                if home != sections - 1:
                    block = lax.ppermute(block, "section", [(sections - 1, home)])
                if finished[cycle] is None:
                    finished[cycle] = block
                else:

                    def keep(*refs, home=home):
                        keep_body(*refs, home=home)

                    finished[cycle] = kernel_call(
                        keep, "keep", shaped(length, width), [VMEM, VMEM]
                    )(finished[cycle], block)
        if tick + 1 < ticks:
            pieces = handed_on(leaving, enters)
    results = [
        kernel_call(
            join_body, "join_output", shaped(length, model_width), [VMEM] * count
        )(*spread(block))
        for block in finished
    ]
    return jnp.stack(results).reshape(hidden_in.shape)


def solution(mesh):
    return jax.shard_map(
        per_device,
        mesh=mesh,
        in_specs=(
            P(None, "section", None, None),
            P("section", None),
            P("section", None, "mp"),
            P("section", None, "mp"),
            P("section", None, "mp"),
            P("section", "mp", None),
            P("section", None),
            P("section", None, "mp"),
            P("section", None, "mp"),
            P("section", "mp", None),
            P(None, "section"),
            P(None, "section"),
        ),
        out_specs=P(None, "section", None, None),
        check_vma=False,
    )
```
